32 devices in a mesh: kpt: 4 (over y, x), grid: 8 (over z, core).
Axes of the slice: x: 2, y: 2, z: 4, core: 2. Of those that a mesh axis runs over, the one named last changes fastest.
Arguments:
- bands: float32 [4, 2, 2, 48, 2304], P('kpt', None, None, 'grid'), may hold values from -6 to 6
- potential: float32 [48, 2304], P('grid'), may hold values from -4 to 4
- phase_numerator_table: int32 [4, 3], P('kpt'), may hold values from 0 to 7
- kweight: float32 [4], P('kpt'), may hold values from 0.25 to 2
- lowest: float32 [4], P('kpt'), may hold values from -6 to -4.5
- cut: float32 [4], P('kpt'), may hold values from 0 to 3
- upper: float32 [4], P('kpt'), may hold values from 15 to 17
- fermi: float32 [1], replicated, may hold values from -0.5 to 1.5
Outputs:
- filtered: float32 [4, 2, 2, 48, 2304], P('kpt', None, None, 'grid')
- band_energies: float32 [4, 2], P('kpt')
- total_energy: float32 [1], replicated
The draws below stay inside these ranges and needn't reach their ends.
All inputs are finite; a program needn't handle non-finite values.
Results may differ from the reference program's by a relative error of at most 0.00022.
Values sent between devices are 32-bit elements; how exact they have to be, the bound alone decides.
A program may use at most 128 MiB of HBM per device.

```python
import math
import jax
import jax.numpy as jnp
from jax import lax

BAND_TOTAL = 2
CELLS_SECOND = 48
CELLS_THIRD = 48
DEGREE = 6
PHASE_DIVISOR = 8
KPOINT_TOTAL = 4
CELLS_FIRST = 48


def plant(drawn, rng, low, high):
    place = [jax.random.randint(jax.random.fold_in(rng, axis), (), 0, length) for axis, length in enumerate(drawn.shape)]
    longest = drawn.shape.index(max(drawn.shape))
    neighbour = place[:longest] + [(place[longest] + 1) % drawn.shape[longest]] + place[longest + 1:]
    return drawn.at[tuple(place)].set(low).at[tuple(neighbour)].set(high)


def levels(key, extent, cuts, low, largest):
    factor_of = 1.0
    for position, shards_of in cuts:
        heights = jax.random.uniform(jax.random.fold_in(jax.random.fold_in(key, 6), position), (shards_of,), jnp.float32, low / len(cuts), largest / len(cuts))
        factor_of = factor_of * jnp.repeat(jnp.exp(heights), extent[position] // shards_of).reshape((-1,) + (1,) * (len(extent) - 1 - position))
    return factor_of


def gaussian(rng, dims, width, most, split=(), kind=jnp.bfloat16):
    values = jax.random.normal(rng, dims, jnp.float32) * width
    if len(split) > 0:
        values = levels(rng, dims, split, -0.22, 0.18) * values
    return jnp.clip(values, min=-most, max=most).astype(kind)


def setup_inputs(seed: int = 0) -> dict:
    streams_of = jax.random.split(jax.random.key(seed), 9)
    bands = gaussian(streams_of[0], (KPOINT_TOTAL, 2, BAND_TOTAL, CELLS_FIRST, CELLS_SECOND * CELLS_THIRD), 1.0, 6.0, ((0, 4), (3, 8)), jnp.float32)
    potential = gaussian(streams_of[1], (CELLS_FIRST, CELLS_SECOND * CELLS_THIRD), 1.0, 4.0, ((0, 8),), jnp.float32)
    phase_numerator_table = plant(jax.random.randint(streams_of[2], (KPOINT_TOTAL, 3), 0, PHASE_DIVISOR), jax.random.fold_in(streams_of[2], 1), 0, PHASE_DIVISOR - 1).astype(jnp.int32)
    kweight = jnp.clip(jnp.exp(math.log(2.0) - 2.0794415 * jax.random.uniform(streams_of[3], (KPOINT_TOTAL,), jnp.float32) ** levels(streams_of[3], (KPOINT_TOTAL,), ((0, 4),), -0.2, 0.2)), 0.25, 2.0)
    lowest = jnp.clip(-6.0 + 1.5 * jax.random.uniform(streams_of[4], (KPOINT_TOTAL,), jnp.float32) ** levels(streams_of[4], (KPOINT_TOTAL,), ((0, 4),), -0.2, 0.2), -6.0, -4.5)
    cut = jnp.clip(3.0 * jax.random.uniform(streams_of[5], (KPOINT_TOTAL,), jnp.float32) ** levels(streams_of[5], (KPOINT_TOTAL,), ((0, 4),), -0.2, 0.2), 0.0, 3.0)
    upper = jnp.clip(15.0 + 2.0 * jax.random.uniform(streams_of[6], (KPOINT_TOTAL,), jnp.float32) ** levels(streams_of[6], (KPOINT_TOTAL,), ((0, 4),), -0.2, 0.2), 15.0, 17.0)
    fermi = jnp.clip(jax.random.uniform(streams_of[7], (1,), jnp.float32, -0.5, 1.5), -0.5, 1.5)
    return dict(bands=bands, potential=potential, phase_numerator_table=phase_numerator_table, kweight=kweight, lowest=lowest, cut=cut, upper=upper, fermi=fermi)


coefficients = (-5369.0 / 1800.0, 12.0 / 7.0, -15.0 / 56.0, 10.0 / 189.0, -1.0 / 112.0, 2.0 / 1925.0, -1.0 / 16632.0)
smearing = 0.5


def twist(part, angle):
    cosine = jnp.cos(angle)
    sine = jnp.sin(angle)
    return jnp.stack([part[0] * cosine - part[1] * sine, part[0] * sine + part[1] * cosine])


def second_diff(extended, axis, length):
    reach = len(coefficients) - 1
    filter_result = coefficients[0] * lax.slice_in_dim(extended, reach, reach + length, axis=axis)
    for offset in range(1, reach + 1):
        upward = lax.slice_in_dim(extended, reach + offset, reach + offset + length, axis=axis)
        downward = lax.slice_in_dim(extended, reach - offset, reach - offset + length, axis=axis)
        filter_result = filter_result + coefficients[offset] * (upward + downward)
    return filter_result


def extend_local(wave_field, axis, angle):
    reach = len(coefficients) - 1
    length = wave_field.shape[axis]
    lower = twist(lax.slice_in_dim(wave_field, length - reach, length, axis=axis), -angle)
    higher = twist(lax.slice_in_dim(wave_field, 0, reach, axis=axis), angle)
    return jnp.concatenate([lower, wave_field, higher], axis=axis)


def apply_h(wave_field, potential, bloch_angles):
    laplace = second_diff(extend_local(wave_field, 2, bloch_angles[0]), 2, wave_field.shape[2])
    laplace = laplace + second_diff(extend_local(wave_field, 3, bloch_angles[1]), 3, wave_field.shape[3])
    laplace = laplace + second_diff(extend_local(wave_field, 4, bloch_angles[2]), 4, wave_field.shape[4])
    return -0.5 * laplace + potential * wave_field


def chebyshev_filter(wave_field, hamiltonian_operator, low_end, cut_end, high_end):
    half_width = (high_end - cut_end) / 2.0
    centre = (high_end + cut_end) / 2.0
    first_sigma = half_width / (low_end - centre)
    sigma = first_sigma
    previous = wave_field
    current = (hamiltonian_operator(wave_field) - centre * wave_field) * (first_sigma / half_width)
    for degree in range(1, DEGREE):
        next_sigma = 1.0 / (2.0 / first_sigma - sigma)
        following = (hamiltonian_operator(current) - centre * current) * (2.0 * next_sigma / half_width) - (sigma * next_sigma) * previous
        previous = current
        current = following
        sigma = next_sigma
    return current


def reference(bands, potential, phase_numerator_table, kweight, lowest, cut, upper, fermi):
    grid_potential = potential.reshape(CELLS_FIRST, CELLS_SECOND, CELLS_THIRD)
    outputs = []
    energies = []
    energy_grand_sum = jnp.zeros((1,), jnp.float32)
    for kpoint_index in range(KPOINT_TOTAL):
        wave_field = bands[kpoint_index].reshape(2, BAND_TOTAL, CELLS_FIRST, CELLS_SECOND, CELLS_THIRD)
        bloch_angles = 2.0 * jnp.pi * phase_numerator_table[kpoint_index].astype(jnp.float32) / PHASE_DIVISOR

        def hamiltonian_operator(value):
            return apply_h(value, grid_potential, bloch_angles)

        filter_result = chebyshev_filter(wave_field, hamiltonian_operator, lowest[kpoint_index], cut[kpoint_index], upper[kpoint_index])
        applied = hamiltonian_operator(filter_result)
        numerator = jnp.sum(filter_result * applied, axis=(0, 2, 3, 4))
        denominator = jnp.sum(filter_result * filter_result, axis=(0, 2, 3, 4))
        band_energy = numerator / denominator
        band_occupation = 1.0 / (1.0 + jnp.exp((band_energy - fermi[0]) / smearing))
        energy_grand_sum = energy_grand_sum + kweight[kpoint_index] * jnp.sum(band_occupation * band_energy)
        outputs.append(filter_result.reshape(2, BAND_TOTAL, CELLS_FIRST, CELLS_SECOND * CELLS_THIRD))
        energies.append(band_energy)
    return jnp.stack(outputs), jnp.stack(energies), energy_grand_sum
```

```python
import functools

import jax
import jax.numpy as jnp
import numpy as np
from jax import lax
from jax.experimental import pallas as pl
from jax.experimental.pallas import tpu as pltpu
from jax.sharding import PartitionSpec as P

SIDE = 48
DEGREE = 6
PHASE_DIVISOR = 8
REACH = 6
LANES = 128
USED = 2 * SIDE
PAD = 8
ROWS = SIDE + 2 * PAD
HALF = SIDE // 2
TILES = SIDE // 8

coefficients = (
    -5369.0 / 1800.0,
    12.0 / 7.0,
    -15.0 / 56.0,
    10.0 / 189.0,
    -1.0 / 112.0,
    2.0 / 1925.0,
    -1.0 / 16632.0,
)
smearing = 0.5
MESH = pl.DeviceIdType.MESH


def third_parts():
    inside = np.zeros((SIDE, SIDE))
    over = np.zeros((SIDE, SIDE))
    under = np.zeros((SIDE, SIDE))
    for z in range(SIDE):
        for j in range(1, REACH + 1):
            weight = -0.5 * coefficients[j]
            for target, sign in ((z + j, 1), (z - j, -1)):
                if 0 <= target < SIDE:
                    inside[target, z] += weight
                elif sign > 0:
                    over[target - SIDE, z] += weight
                else:
                    under[target + SIDE, z] += weight
    plain = np.zeros((LANES, LANES))
    cosine = np.zeros((LANES, LANES))
    sine = np.zeros((LANES, LANES))
    both, apart = over + under, over - under
    for c in range(2):
        s = slice(c * SIDE, (c + 1) * SIDE)
        plain[s, s] = inside
        cosine[s, s] = both
    re, im = slice(0, SIDE), slice(SIDE, USED)
    sine[im, re] = -apart
    sine[re, im] = apart
    return [a.astype(np.float32) for a in (plain, cosine, sine)]


def kernel(
    n,
    members_k,
    scal_ref,
    packed_ref,
    pot_ref,
    mat_ref,
    out_ref,
    energy_ref,
    total_ref,
    field,
    potential,
    gathered,
    gathered_pot,
    part,
    part_k,
    send,
    recv,
    send_pot,
    recv_pot,
    send_red,
    recv_red,
    send_k,
    recv_k,
    swap_sem,
):
    planes = REACH
    chips = n // 2
    blocks = n
    home = (blocks - 2) // 2
    me = lax.axis_index("grid")
    kpt = lax.axis_index("kpt")
    chip, core = me // 2, me % 2
    partner = chip * 2 + (1 - core)

    barrier = pltpu.get_barrier_semaphore()
    for d in range(1, n):
        pl.semaphore_signal(barrier, inc=1, device_id=(kpt, (me + d) % n), device_id_type=MESH)
    for d in range(1, members_k):
        pl.semaphore_signal(
            barrier, inc=1, device_id=((kpt + d) % members_k, me), device_id_type=MESH
        )
    pl.semaphore_wait(barrier, n - 1 + members_k - 1)

    def remote(src, dst, ssem, rsem, target):
        return pltpu.make_async_remote_copy(
            src_ref=src,
            dst_ref=dst,
            send_sem=ssem,
            recv_sem=rsem,
            device_id=(kpt, target),
            device_id_type=MESH,
        )

    has_up, has_down = chip < chips - 1, chip > 0

    def own(which, ssem, target):
        return remote(packed_ref.at[which], gathered.at[me], ssem, recv.at[me], target)

    def own_pot(ssem, target):
        return remote(pot_ref, gathered_pot.at[me], ssem, recv_pot.at[me], target)

    @pl.when(has_up)
    def _():
        own(core, send.at[0], me + 2).start()
        own(1 - core, send.at[1], partner + 2).start()
        own_pot(send_pot.at[0], me + 2).start()

    @pl.when(has_down)
    def _():
        own(core, send.at[2], me - 2).start()
        own(1 - core, send.at[3], partner - 2).start()
        own_pot(send_pot.at[1], me - 2).start()

    own(1 - core, send.at[4], partner).start()
    own_pot(send_pot.at[2], partner).start()

    lane = lax.broadcasted_iota(jnp.int32, (8, LANES), 1)
    first = lane < SIDE
    used = lane < USED
    zero = jnp.zeros((8, LANES), jnp.float32)

    def turn(v, cosine, sine):
        other = jnp.where(first, pltpu.roll(v, LANES - SIDE, 1), pltpu.roll(v, SIDE, 1))
        signed = jnp.where(used, jnp.where(first, -sine, sine), 0.0)
        return cosine * v + signed * other

    cos_x, sin_x = scal_ref[0], scal_ref[1]
    cos_y, sin_y = scal_ref[2], scal_ref[3]

    def put(slot, plane, t, v):
        field[slot, plane, pl.ds(PAD + 8 * t, 8), :] = v
        if t == 0:
            field[slot, plane, pl.ds(PAD + SIDE, 8), :] = turn(v, cos_y, sin_y)
        if t == TILES - 1:
            field[slot, plane, pl.ds(0, 8), :] = turn(v, cos_y, -sin_y)

    def unpack(load, slab):
        place = lax.rem(slab - 2 * chip + home + blocks, blocks)
        absolute = 2 * chip - home + place
        wrapped_low = absolute < 0
        wrapped_high = absolute >= blocks
        base = planes + place * planes

        def emit(change):
            for hp in range(2 * planes):
                plane, half = hp // 2, hp % 2
                for r in range(HALF // 8):
                    if hp < 9:
                        v = jnp.where(used, load(hp, r), zero)
                    else:
                        g = hp - 9
                        v = zero
                        for q in range(3):
                            piece = pltpu.roll(load(3 * g + q, r), 32 + 32 * q, 1)
                            inside = (lane >= 32 * q) & (lane < 32 * q + 32)
                            v = jnp.where(inside, piece, v)
                    put(0, base + plane, half * (HALF // 8) + r, change(v))

        sine = jnp.where(wrapped_low, -sin_x, sin_x)
        sine = jnp.where(wrapped_low | wrapped_high, sine, 0.0)
        cosine = jnp.where(wrapped_low | wrapped_high, cos_x, 1.0)
        emit(lambda v: turn(v, cosine, sine))

    def unpack_pot(load, slab):
        place = lax.rem(slab - 2 * chip + home + blocks, blocks)
        for pair in range(planes // 2):
            for t in range(TILES):
                v = load(pair, t) - 1.5 * coefficients[0]
                swap_up = pltpu.roll(v, SIDE, 1)
                swap_down = pltpu.roll(v, LANES - SIDE, 1)
                rows = pl.ds(8 * t, 8)
                potential[place * planes + 2 * pair, rows, :] = jnp.where(first, v, swap_up)
                potential[place * planes + 2 * pair + 1, rows, :] = jnp.where(first, swap_down, v)

    def own_load(hp, r):
        return packed_ref[core, hp, pl.ds(8 * r, 8), :]

    unpack(own_load, me)
    unpack_pot(lambda pair, t: pot_ref[pair, pl.ds(8 * t, 8), :], me)

    def unpack_slab(slab):
        unpack(lambda hp, r: gathered[slab, hp, pl.ds(8 * r, 8), :], slab)

    def unpack_pot_slab(slab):
        unpack_pot(lambda pair, t: gathered_pot[slab, pair, pl.ds(8 * t, 8), :], slab)

    def await_slab(slab):
        remote(gathered.at[slab], gathered.at[slab], send.at[0], recv.at[slab], partner).wait_recv()

    def await_pot(slab):
        remote(
            gathered_pot.at[slab], gathered_pot.at[slab], send_pot.at[0], recv_pot.at[slab], partner
        ).wait_recv()

    def relay(slab, target):
        return remote(
            gathered.at[slab], gathered.at[slab], send.at[5 + slab], recv.at[slab], target
        )

    def relay_pot(slab, target, side):
        return remote(
            gathered_pot.at[slab],
            gathered_pot.at[slab],
            send_pot.at[3 + 2 * slab + side],
            recv_pot.at[slab],
            target,
        )

    def arrive(source, onward, target):
        for p in range(2):
            slab = 2 * source + p
            await_slab(slab)

            @pl.when(onward)
            def _():
                relay(slab, target).start()

        same = 2 * source + core
        await_pot(same)

        @pl.when(onward)
        def _():
            relay_pot(same, target, 0).start()

        relay_pot(same, partner, 1).start()

    def process(source):
        def one(p, carry):
            slab = 2 * source + p
            unpack_slab(slab)
            return carry

        lax.fori_loop(0, 2, one, 0)
        unpack_pot_slab(2 * source + core)

    def gather_step(d, carry):
        low_there, high_there = chip - d >= 0, chip + d < chips

        @pl.when(low_there)
        def _():
            arrive(chip - d, has_up, me + 2)

        @pl.when(high_there)
        def _():
            arrive(chip + d, has_down, me - 2)

        @pl.when(low_there)
        def _():
            process(chip - d)

        @pl.when(high_there)
        def _():
            process(chip + d)

        return carry

    await_slab(partner)
    unpack_slab(partner)
    await_pot(partner)
    unpack_pot_slab(partner)
    lax.fori_loop(1, chips, gather_step, 0)

    def other_pot(source, carry):
        @pl.when(source != chip)
        def _():
            slab = 2 * source + (1 - core)
            await_pot(slab)
            unpack_pot_slab(slab)

        return carry

    lax.fori_loop(0, chips, other_pot, 0)

    def wrap_planes(slot):
        def one(i, carry):
            for t in range(ROWS // 8):
                rows = pl.ds(8 * t, 8)
                low = field[slot, blocks * planes + i, rows, :]
                field[slot, i, rows, :] = turn(low, cos_x, -sin_x)
                high = field[slot, planes + i, rows, :]
                field[slot, planes + blocks * planes + i, rows, :] = turn(high, cos_x, sin_x)
            return carry

        lax.fori_loop(0, planes, one, 0)

    wrap_planes(0)
    weights = [-0.5 * c for c in coefficients]

    def step(m, carry):
        now = lax.rem(m - 1, 3)
        new = lax.rem(m, 3)
        old = jnp.where(m == 1, now, lax.rem(m + 1, 3))
        gain, centre, back = scal_ref[3 * m + 1], scal_ref[3 * m + 2], scal_ref[3 * m + 3]
        low = jnp.maximum(0, m - (DEGREE + 1) + home)

        def block(k, inner):
            base = k * planes
            middle = [field[now, base + planes + p, pl.ds(PAD, SIDE), :] for p in range(planes)]
            rows = jnp.concatenate(middle, axis=0)
            high = rows.astype(jnp.bfloat16)
            rest = (rows - high.astype(jnp.float32)).astype(jnp.bfloat16)
            both = jnp.concatenate([high, rest], axis=1)
            third = jnp.dot(both, mat_ref[...], preferred_element_type=jnp.float32)
            third = third[:, :LANES] + third[:, LANES:]
            for t in range(TILES):
                window = [
                    field[now, base + i, pl.ds(PAD + 8 * t, 8), :] for i in range(3 * planes)
                ]
                for p in range(planes):
                    centre_value = window[planes + p]
                    total = third[p * SIDE + 8 * t : p * SIDE + 8 * t + 8, :]
                    total = total + centre_value * (
                        potential[base + p, pl.ds(8 * t, 8), :] - centre
                    )
                    for j in range(1, REACH + 1):
                        around = window[planes + p + j] + window[planes + p - j]
                        above = field[now, base + planes + p, pl.ds(PAD + 8 * t + j, 8), :]
                        below = field[now, base + planes + p, pl.ds(PAD + 8 * t - j, 8), :]
                        total = total + weights[j] * (around + (above + below))
                    previous = field[old, base + planes + p, pl.ds(PAD + 8 * t, 8), :]
                    put(new, base + planes + p, t, gain * total - back * previous)
            return inner

        lax.fori_loop(low, blocks - low, block, 0)

        @pl.when(m - DEGREE + home <= 0)
        def _():
            wrap_planes(new)

        return carry

    lax.fori_loop(1, DEGREE + 2, step, 0)
    slot, applied = DEGREE % 3, (DEGREE + 1) % 3

    mine = planes + (home + core) * planes
    theirs = planes + (home + 1 - core) * planes
    body = pl.ds(PAD, SIDE)
    swap = remote(
        field.at[slot, pl.ds(theirs, planes), body, :],
        out_ref.at[core],
        swap_sem.at[0],
        swap_sem.at[1],
        partner,
    )
    swap.start()

    def sums(i, carry):
        top, bottom = carry
        plane = planes + home * planes + i
        for t in range(TILES):
            f = field[slot, plane, pl.ds(PAD + 8 * t, 8), :]
            top = top + f * field[applied, plane, pl.ds(PAD + 8 * t, 8), :]
            bottom = bottom + f * f
        return top, bottom

    top, bottom = lax.fori_loop(0, 2 * planes, sums, (zero, zero))
    part[me, 0] = jnp.broadcast_to(jnp.sum(top, keepdims=True), (8, LANES))
    part[me, 1] = jnp.broadcast_to(jnp.sum(bottom, keepdims=True), (8, LANES))

    def reduction(d):
        return remote(
            part.at[me], part.at[me], send_red.at[d], recv_red.at[me], lax.rem(me + d, n)
        )

    for d in range(1, n):
        reduction(d).start()
    for i in range(planes):
        for t in range(TILES):
            out_ref[core, i, pl.ds(8 * t, 8), :] = field[slot, mine + i, pl.ds(PAD + 8 * t, 8), :]
    for d in range(1, n):
        source = lax.rem(me + d, n)
        remote(
            part.at[source], part.at[source], send_red.at[d], recv_red.at[source], source
        ).wait_recv()
    kweight, fermi = scal_ref[3 * DEGREE + 7], scal_ref[3 * DEGREE + 8]
    term = zero
    for b in range(2):
        numerator, denominator = zero, zero
        for c in range(chips):
            numerator = numerator + part[2 * c + b, 0]
            denominator = denominator + part[2 * c + b, 1]
        energy = numerator / denominator
        energy_ref[b] = energy
        term = term + energy / (1.0 + jnp.exp((energy - fermi) / smearing))
    part_k[kpt] = kweight * term

    def across(d):
        return pltpu.make_async_remote_copy(
            src_ref=part_k.at[kpt],
            dst_ref=part_k.at[kpt],
            send_sem=send_k.at[d],
            recv_sem=recv_k.at[kpt],
            device_id=(lax.rem(kpt + d, members_k), me),
            device_id_type=MESH,
        )

    for d in range(1, members_k):
        across(d).start()
    for d in range(1, members_k):
        source = lax.rem(kpt + d, members_k)
        pltpu.make_async_remote_copy(
            src_ref=part_k.at[source],
            dst_ref=part_k.at[source],
            send_sem=send_k.at[d],
            recv_sem=recv_k.at[source],
            device_id=(source, me),
            device_id_type=MESH,
        ).wait_recv()
    grand = zero
    for k in range(members_k):
        grand = grand + part_k[k]
    total_ref[...] = grand

    swap.wait()
    for d in range(1, n):
        reduction(d).wait_send()
    for d in range(1, members_k):
        across(d).wait_send()

    @pl.when(has_up)
    def _():
        own(core, send.at[0], me + 2).wait_send()
        own(1 - core, send.at[1], partner + 2).wait_send()
        own_pot(send_pot.at[0], me + 2).wait_send()

    @pl.when(has_down)
    def _():
        own(core, send.at[2], me - 2).wait_send()
        own(1 - core, send.at[3], partner - 2).wait_send()
        own_pot(send_pot.at[1], me - 2).wait_send()

    own(1 - core, send.at[4], partner).wait_send()
    own_pot(send_pot.at[2], partner).wait_send()

    def drain(source, carry):
        @pl.when(source != chip)
        def _():
            onward = jnp.where(source < chip, has_up, has_down)
            target = jnp.where(source < chip, me + 2, me - 2)

            @pl.when(onward)
            def _():
                relay(2 * source, target).wait_send()
                relay(2 * source + 1, target).wait_send()
                relay_pot(2 * source + core, target, 0).wait_send()

            relay_pot(2 * source + core, partner, 1).wait_send()

        return carry

    lax.fori_loop(0, chips, drain, 0)


def per_device(bands, potential, table, kweight, lowest, cut, upper, fermi):
    n = lax.axis_size("grid")
    members_k = lax.axis_size("kpt")
    planes = bands.shape[3]
    angles = 2.0 * jnp.pi * table[0].astype(jnp.float32) / PHASE_DIVISOR
    cosines, sines = jnp.cos(angles), jnp.sin(angles)

    half_width = (upper[0] - cut[0]) / 2.0
    centre = (upper[0] + cut[0]) / 2.0
    first_sigma = half_width / (lowest[0] - centre)
    sigma = first_sigma
    nothing = jnp.zeros((), jnp.float32)
    scalars = [cosines[0], sines[0], cosines[1], sines[1]]
    scalars += [first_sigma / half_width, centre, nothing]
    for degree in range(1, DEGREE):
        next_sigma = 1.0 / (2.0 / first_sigma - sigma)
        scalars += [2.0 * next_sigma / half_width, centre, sigma * next_sigma]
        sigma = next_sigma
    scalars += [nothing + 1.0, nothing, nothing, kweight[0], fermi[0]]
    scalars = jnp.stack(scalars)

    plain, cosine, sine = third_parts()
    matrix = plain + cosines[2] * cosine + sines[2] * sine
    rounded = lax.reduce_precision(matrix, 8, 7)
    high = rounded.astype(jnp.bfloat16)
    rest = (matrix - rounded).astype(jnp.bfloat16)
    matrix = jnp.concatenate(
        [
            jnp.concatenate([high, rest], axis=1),
            jnp.concatenate([high, jnp.zeros_like(high)], axis=1),
        ],
        axis=0,
    )

    waves = bands[0].reshape(2, 2, planes, SIDE, SIDE).transpose(1, 2, 3, 0, 4)
    waves = waves.reshape(2, 2 * planes, HALF, USED)
    head, tail = waves[:, :9], waves[:, 9:]
    tail = tail.reshape(2, 3, HALF, 3, 32).transpose(0, 1, 3, 2, 4).reshape(2, 9, HALF, 32)
    packed = jnp.concatenate([head, tail], axis=-1)

    pairs = potential.reshape(planes // 2, 2, SIDE, SIDE).transpose(0, 2, 1, 3)
    pairs = pairs.reshape(planes // 2, SIDE, USED)
    pairs = jnp.pad(pairs, ((0, 0), (0, 0), (0, LANES - USED)))

    vmem = pl.BlockSpec(memory_space=pltpu.VMEM)
    total_planes = n * planes
    dma = pltpu.SemaphoreType.DMA
    out, energy, total = pl.pallas_call(
        functools.partial(kernel, n, members_k),
        name="cheb",
        out_shape=(
            jax.ShapeDtypeStruct((2, planes, SIDE, LANES), jnp.float32),
            jax.ShapeDtypeStruct((2, 8, LANES), jnp.float32),
            jax.ShapeDtypeStruct((8, LANES), jnp.float32),
        ),
        in_specs=[pl.BlockSpec(memory_space=pltpu.SMEM), vmem, vmem, vmem],
        out_specs=(vmem, vmem, vmem),
        scratch_shapes=[
            pltpu.VMEM((3, total_planes + 2 * planes, ROWS, LANES), jnp.float32),
            pltpu.VMEM((total_planes, SIDE, LANES), jnp.float32),
            pltpu.VMEM((n, 9, HALF, LANES), jnp.float32),
            pltpu.VMEM((n, planes // 2, SIDE, LANES), jnp.float32),
            pltpu.VMEM((n, 2, 8, LANES), jnp.float32),
            pltpu.VMEM((members_k, 8, LANES), jnp.float32),
            dma((5 + n,)),
            dma((n,)),
            dma((3 + 2 * n,)),
            dma((n,)),
            dma((n,)),
            dma((n,)),
            dma((members_k,)),
            dma((members_k,)),
            dma((2,)),
        ],
        compiler_params=pltpu.CompilerParams(
            collective_id=0, has_side_effects=True, vmem_limit_bytes=56 * 1024 * 1024
        ),
    )(scalars, packed, pairs, matrix)
    filtered = out[..., :USED].reshape(2, planes, SIDE, 2, SIDE).transpose(3, 0, 1, 2, 4)
    filtered = filtered.reshape(1, 2, 2, planes, SIDE * SIDE)
    return filtered, energy[:, 0, 0][None], total[0, :1]


def solution(mesh):
    in_specs = (
        P("kpt", None, None, "grid", None),
        P("grid", None),
        P("kpt", None),
        P("kpt"),
        P("kpt"),
        P("kpt"),
        P("kpt"),
        P(),
    )
    out_specs = (P("kpt", None, None, "grid", None), P("kpt", None), P())
    return jax.shard_map(
        per_device, mesh=mesh, in_specs=in_specs, out_specs=out_specs, check_vma=False
    )
```

```python
import functools

import jax
import jax.numpy as jnp
import numpy as np
from jax import lax
from jax.experimental import pallas as pl
from jax.experimental.pallas import tpu as pltpu
from jax.sharding import PartitionSpec as P

SIDE = 48
DEGREE = 6
PHASE_DIVISOR = 8
REACH = 6
LANES = 128
USED = 2 * SIDE
PAD = 8
ROWS = SIDE + 2 * PAD
HALF = SIDE // 2
TILES = SIDE // 8

coefficients = (
    -5369.0 / 1800.0,
    12.0 / 7.0,
    -15.0 / 56.0,
    10.0 / 189.0,
    -1.0 / 112.0,
    2.0 / 1925.0,
    -1.0 / 16632.0,
)
smearing = 0.5
MESH = pl.DeviceIdType.MESH


def third_parts():
    inside = np.zeros((SIDE, SIDE))
    over = np.zeros((SIDE, SIDE))
    under = np.zeros((SIDE, SIDE))
    for z in range(SIDE):
        for j in range(1, REACH + 1):
            weight = -0.5 * coefficients[j]
            for target, sign in ((z + j, 1), (z - j, -1)):
                if 0 <= target < SIDE:
                    inside[target, z] += weight
                elif sign > 0:
                    over[target - SIDE, z] += weight
                else:
                    under[target + SIDE, z] += weight
    plain = np.zeros((LANES, LANES))
    cosine = np.zeros((LANES, LANES))
    sine = np.zeros((LANES, LANES))
    both, apart = over + under, over - under
    for c in range(2):
        s = slice(c * SIDE, (c + 1) * SIDE)
        plain[s, s] = inside
        cosine[s, s] = both
    re, im = slice(0, SIDE), slice(SIDE, USED)
    sine[im, re] = -apart
    sine[re, im] = apart
    return [a.astype(np.float32) for a in (plain, cosine, sine)]


def kernel(
    n,
    members_k,
    table_ref,
    kweight_ref,
    lowest_ref,
    cut_ref,
    upper_ref,
    fermi_ref,
    packed_ref,
    pot_ref,
    parts_ref,
    out_ref,
    energy_ref,
    total_ref,
    field_0,
    field_1,
    field_2,
    mat_ref,
    potential,
    gathered,
    gathered_pot,
    part,
    part_k,
    send,
    recv,
    send_pot,
    recv_pot,
    send_red,
    recv_red,
    send_k,
    recv_k,
    swap_sem,
):
    planes = REACH
    chips = n // 2
    blocks = n
    home = (blocks - 2) // 2
    me = lax.axis_index("grid")
    kpt = lax.axis_index("kpt")
    chip, core = me // 2, me % 2
    partner = chip * 2 + (1 - core)

    barrier = pltpu.get_barrier_semaphore()
    for d in range(1, n):
        pl.semaphore_signal(barrier, inc=1, device_id=(kpt, (me + d) % n), device_id_type=MESH)
    for d in range(1, members_k):
        pl.semaphore_signal(
            barrier, inc=1, device_id=((kpt + d) % members_k, me), device_id_type=MESH
        )
    pl.semaphore_wait(barrier, n - 1 + members_k - 1)

    def remote(src, dst, ssem, rsem, target):
        return pltpu.make_async_remote_copy(
            src_ref=src,
            dst_ref=dst,
            send_sem=ssem,
            recv_sem=rsem,
            device_id=(kpt, target),
            device_id_type=MESH,
        )

    has_up, has_down = chip < chips - 1, chip > 0

    def own(which, ssem, target):
        return remote(packed_ref.at[which], gathered.at[me], ssem, recv.at[me], target)

    def own_pot(ssem, target):
        return remote(pot_ref, gathered_pot.at[me], ssem, recv_pot.at[me], target)

    @pl.when(has_up)
    def _():
        own(core, send.at[0], me + 2).start()
        own(1 - core, send.at[1], partner + 2).start()
        own_pot(send_pot.at[0], me + 2).start()

    @pl.when(has_down)
    def _():
        own(core, send.at[2], me - 2).start()
        own(1 - core, send.at[3], partner - 2).start()
        own_pot(send_pot.at[1], me - 2).start()

    own(1 - core, send.at[4], partner).start()
    own_pot(send_pot.at[2], partner).start()

    lane = lax.broadcasted_iota(jnp.int32, (8, LANES), 1)
    first = lane < SIDE
    used = lane < USED
    zero = jnp.zeros((8, LANES), jnp.float32)

    def turn(v, cosine, sine):
        other = jnp.where(first, pltpu.roll(v, LANES - SIDE, 1), pltpu.roll(v, SIDE, 1))
        signed = jnp.where(used, jnp.where(first, -sine, sine), 0.0)
        return cosine * v + signed * other

    def spread(scalar):
        return jnp.full((8, LANES), scalar)

    def phase(d):
        numerator = spread(table_ref[0, d])
        cosine, sine = jnp.ones((8, LANES), jnp.float32), zero
        for i in range(1, PHASE_DIVISOR):
            here = numerator == i
            angle = 2.0 * np.pi * i / PHASE_DIVISOR
            cosine = jnp.where(here, float(np.cos(angle)), cosine)
            sine = jnp.where(here, float(np.sin(angle)), sine)
        return cosine, sine

    cos_x, sin_x = phase(0)
    cos_y, sin_y = phase(1)
    cos_z, sin_z = phase(2)
    low_end, cut_end, high_end = (spread(r[0]) for r in (lowest_ref, cut_ref, upper_ref))
    half_width = (high_end - cut_end) / 2.0
    centre = (high_end + cut_end) / 2.0
    first_sigma = half_width / (low_end - centre)
    sigma = first_sigma
    recurrence = [(first_sigma / half_width, None)]
    for degree in range(1, DEGREE):
        next_sigma = 1.0 / (2.0 / first_sigma - sigma)
        recurrence.append((2.0 * next_sigma / half_width, sigma * next_sigma))
        sigma = next_sigma

    for r in range(LANES // 16):
        rows = pl.ds(16 * r, 16)
        cosine = jnp.concatenate([cos_z, cos_z], axis=0)
        sine = jnp.concatenate([sin_z, sin_z], axis=0)
        entry = parts_ref[0, rows, :] + cosine * parts_ref[1, rows, :] + sine * parts_ref[2, rows, :]
        high = entry.astype(jnp.bfloat16)
        rest = (entry - high.astype(jnp.float32)).astype(jnp.bfloat16)
        lower = pl.ds(LANES + 16 * r, 16)
        mat_ref[rows, pl.ds(0, LANES)] = high
        mat_ref[rows, pl.ds(LANES, LANES)] = rest
        mat_ref[lower, pl.ds(0, LANES)] = high
        mat_ref[lower, pl.ds(LANES, LANES)] = jnp.zeros_like(high)

    fields = (field_0, field_1, field_2)

    def put(field, plane, t, v):
        field[plane, pl.ds(PAD + 8 * t, 8), :] = v
        if t == 0:
            field[plane, pl.ds(PAD + SIDE, 8), :] = turn(v, cos_y, sin_y)
        if t == TILES - 1:
            field[plane, pl.ds(0, 8), :] = turn(v, cos_y, -sin_y)

    def unpack(load, slab):
        place = lax.rem(slab - 2 * chip + home + blocks, blocks)
        absolute = 2 * chip - home + place
        wrapped_low = absolute < 0
        wrapped_high = absolute >= blocks
        base = planes + place * planes

        def emit(change):
            for hp in range(2 * planes):
                plane, half = hp // 2, hp % 2
                for r in range(HALF // 8):
                    if hp < 9:
                        v = jnp.where(used, load(hp, r), zero)
                    else:
                        g = hp - 9
                        v = zero
                        for q in range(3):
                            piece = pltpu.roll(load(3 * g + q, r), 32 + 32 * q, 1)
                            inside = (lane >= 32 * q) & (lane < 32 * q + 32)
                            v = jnp.where(inside, piece, v)
                    put(field_0, base + plane, half * (HALF // 8) + r, change(v))

        wrapped = wrapped_low | wrapped_high

        @pl.when(wrapped)
        def _():
            way = jnp.where(wrapped_low, -1.0, 1.0)
            emit(lambda v: turn(v, cos_x, way * sin_x))

        @pl.when(jnp.logical_not(wrapped))
        def _():
            emit(lambda v: v)

    def unpack_pot(load, slab):
        place = lax.rem(slab - 2 * chip + home + blocks, blocks)
        for pair in range(planes // 2):
            for t in range(TILES):
                v = load(pair, t) - 1.5 * coefficients[0]
                swap_up = pltpu.roll(v, SIDE, 1)
                swap_down = pltpu.roll(v, LANES - SIDE, 1)
                rows = pl.ds(8 * t, 8)
                potential[place * planes + 2 * pair, rows, :] = jnp.where(first, v, swap_up)
                potential[place * planes + 2 * pair + 1, rows, :] = jnp.where(first, swap_down, v)

    def own_load(hp, r):
        return packed_ref[core, hp, pl.ds(8 * r, 8), :]

    unpack(own_load, me)
    unpack_pot(lambda pair, t: pot_ref[pair, pl.ds(8 * t, 8), :], me)

    def unpack_slab(slab):
        unpack(lambda hp, r: gathered[slab, hp, pl.ds(8 * r, 8), :], slab)

    def unpack_pot_slab(slab):
        unpack_pot(lambda pair, t: gathered_pot[slab, pair, pl.ds(8 * t, 8), :], slab)

    def await_slab(slab):
        remote(gathered.at[slab], gathered.at[slab], send.at[0], recv.at[slab], partner).wait_recv()

    def await_pot(slab):
        remote(
            gathered_pot.at[slab], gathered_pot.at[slab], send_pot.at[0], recv_pot.at[slab], partner
        ).wait_recv()

    def relay(slab, target):
        return remote(
            gathered.at[slab], gathered.at[slab], send.at[5 + slab], recv.at[slab], target
        )

    def relay_pot(slab, target, side):
        return remote(
            gathered_pot.at[slab],
            gathered_pot.at[slab],
            send_pot.at[3 + 2 * slab + side],
            recv_pot.at[slab],
            target,
        )

    def arrive(source, onward, target):
        for p in range(2):
            slab = 2 * source + p
            await_slab(slab)

            @pl.when(onward)
            def _():
                relay(slab, target).start()

        same = 2 * source + core
        await_pot(same)

        @pl.when(onward)
        def _():
            relay_pot(same, target, 0).start()

        relay_pot(same, partner, 1).start()

    def process(source):
        def one(p, carry):
            slab = 2 * source + p
            unpack_slab(slab)
            return carry

        lax.fori_loop(0, 2, one, 0)
        unpack_pot_slab(2 * source + core)

    def gather_step(d, carry):
        low_there, high_there = chip - d >= 0, chip + d < chips

        @pl.when(low_there)
        def _():
            arrive(chip - d, has_up, me + 2)

        @pl.when(high_there)
        def _():
            arrive(chip + d, has_down, me - 2)

        @pl.when(low_there)
        def _():
            process(chip - d)

        @pl.when(high_there)
        def _():
            process(chip + d)

        return carry

    await_slab(partner)
    unpack_slab(partner)
    await_pot(partner)
    unpack_pot_slab(partner)
    lax.fori_loop(1, chips, gather_step, 0)

    def other_pot(source, carry):
        @pl.when(source != chip)
        def _():
            slab = 2 * source + (1 - core)
            await_pot(slab)
            unpack_pot_slab(slab)

        return carry

    lax.fori_loop(0, chips, other_pot, 0)

    def wrap_planes(field):
        def one(i, carry):
            tiles = [pl.ds(8 * t, 8) for t in range(ROWS // 8)]
            lows = [field[blocks * planes + i, rows, :] for rows in tiles]
            highs = [field[planes + i, rows, :] for rows in tiles]
            lows = [turn(v, cos_x, -sin_x) for v in lows]
            highs = [turn(v, cos_x, sin_x) for v in highs]
            for rows, low, high in zip(tiles, lows, highs):
                field[i, rows, :] = low
                field[planes + blocks * planes + i, rows, :] = high
            return carry

        lax.fori_loop(0, planes, one, 0)

    wrap_planes(field_0)
    weights = [-0.5 * c for c in coefficients]

    def apply(m, k):
        field = fields[(m - 1) % 3]
        base = k * planes
        middle = [field[base + planes + p, pl.ds(PAD, SIDE), :] for p in range(planes)]
        rows = jnp.concatenate(middle, axis=0)
        high = rows.astype(jnp.bfloat16)
        rest = (rows - high.astype(jnp.float32)).astype(jnp.bfloat16)
        both = jnp.concatenate([high, rest], axis=1)
        third = jnp.dot(both, mat_ref[...], preferred_element_type=jnp.float32)
        third = third[:, :LANES] + third[:, LANES:]
        for t in range(TILES):
            tile = pl.ds(PAD + 8 * t, 8)
            window = [field[base + i, tile, :] for i in range(3 * planes)]
            for p in range(planes):
                value = window[planes + p]
                total = third[p * SIDE + 8 * t : p * SIDE + 8 * t + 8, :]
                shift = potential[base + p, pl.ds(8 * t, 8), :]
                if m <= DEGREE:
                    shift = shift - centre
                total = total + value * shift
                for j in range(1, REACH + 1):
                    around = window[planes + p + j] + window[planes + p - j]
                    above = field[base + planes + p, pl.ds(PAD + 8 * t + j, 8), :]
                    below = field[base + planes + p, pl.ds(PAD + 8 * t - j, 8), :]
                    total = total + weights[j] * (around + (above + below))
                yield base + planes + p, t, tile, value, total

    for m in range(1, DEGREE + 1):
        gain, back = recurrence[m - 1]
        low = max(0, m - (DEGREE + 1) + home)

        def block(k, carry, m=m, gain=gain, back=back):
            for plane, t, tile, _, total in apply(m, k):
                following = gain * total
                if back is not None:
                    following = following - back * fields[(m + 1) % 3][plane, tile, :]
                put(fields[m % 3], plane, t, following)
            return carry

        lax.fori_loop(low, blocks - low, block, 0)
        if m - DEGREE + home <= 0:
            wrap_planes(fields[m % 3])
    final = fields[DEGREE % 3]

    mine = planes + (home + core) * planes
    theirs = planes + (home + 1 - core) * planes
    body = pl.ds(PAD, SIDE)
    swap = remote(
        final.at[pl.ds(theirs, planes), body, :],
        out_ref.at[core],
        swap_sem.at[0],
        swap_sem.at[1],
        partner,
    )
    swap.start()

    def sums(k, carry):
        tops, bottoms = list(carry[0]), list(carry[1])
        for plane, t, _, value, total in apply(DEGREE + 1, k):
            tops[t % 2] = tops[t % 2] + value * total
            bottoms[t % 2] = bottoms[t % 2] + value * value
        return tuple(tops), tuple(bottoms)

    tops, bottoms = lax.fori_loop(home, blocks - home, sums, ((zero, zero), (zero, zero)))
    top, bottom = tops[0] + tops[1], bottoms[0] + bottoms[1]
    part[me, 0] = jnp.broadcast_to(jnp.sum(top, keepdims=True), (8, LANES))
    part[me, 1] = jnp.broadcast_to(jnp.sum(bottom, keepdims=True), (8, LANES))

    def reduction(d):
        return remote(
            part.at[me], part.at[me], send_red.at[d], recv_red.at[me], lax.rem(me + d, n)
        )

    for d in range(1, n):
        reduction(d).start()
    for i in range(planes):
        for t in range(TILES):
            out_ref[core, i, pl.ds(8 * t, 8), :] = final[mine + i, pl.ds(PAD + 8 * t, 8), :]
    for d in range(1, n):
        source = lax.rem(me + d, n)
        remote(
            part.at[source], part.at[source], send_red.at[d], recv_red.at[source], source
        ).wait_recv()
    kweight, fermi = kweight_ref[0], fermi_ref[0]
    term = zero
    for b in range(2):
        numerator, denominator = zero, zero
        for c in range(chips):
            numerator = numerator + part[2 * c + b, 0]
            denominator = denominator + part[2 * c + b, 1]
        energy = numerator / denominator
        energy_ref[b] = energy
        term = term + energy / (1.0 + jnp.exp((energy - fermi) / smearing))
    part_k[kpt] = kweight * term

    def across(d):
        return pltpu.make_async_remote_copy(
            src_ref=part_k.at[kpt],
            dst_ref=part_k.at[kpt],
            send_sem=send_k.at[d],
            recv_sem=recv_k.at[kpt],
            device_id=(lax.rem(kpt + d, members_k), me),
            device_id_type=MESH,
        )

    for d in range(1, members_k):
        across(d).start()
    for d in range(1, members_k):
        source = lax.rem(kpt + d, members_k)
        pltpu.make_async_remote_copy(
            src_ref=part_k.at[source],
            dst_ref=part_k.at[source],
            send_sem=send_k.at[d],
            recv_sem=recv_k.at[source],
            device_id=(source, me),
            device_id_type=MESH,
        ).wait_recv()
    grand = zero
    for k in range(members_k):
        grand = grand + part_k[k]
    total_ref[...] = grand

    swap.wait()
    for d in range(1, n):
        reduction(d).wait_send()
    for d in range(1, members_k):
        across(d).wait_send()

    @pl.when(has_up)
    def _():
        own(core, send.at[0], me + 2).wait_send()
        own(1 - core, send.at[1], partner + 2).wait_send()
        own_pot(send_pot.at[0], me + 2).wait_send()

    @pl.when(has_down)
    def _():
        own(core, send.at[2], me - 2).wait_send()
        own(1 - core, send.at[3], partner - 2).wait_send()
        own_pot(send_pot.at[1], me - 2).wait_send()

    own(1 - core, send.at[4], partner).wait_send()
    own_pot(send_pot.at[2], partner).wait_send()

    def drain(source, carry):
        @pl.when(source != chip)
        def _():
            onward = jnp.where(source < chip, has_up, has_down)
            target = jnp.where(source < chip, me + 2, me - 2)

            @pl.when(onward)
            def _():
                relay(2 * source, target).wait_send()
                relay(2 * source + 1, target).wait_send()
                relay_pot(2 * source + core, target, 0).wait_send()

            relay_pot(2 * source + core, partner, 1).wait_send()

        return carry

    lax.fori_loop(0, chips, drain, 0)


def per_device(bands, potential, table, kweight, lowest, cut, upper, fermi):
    n = lax.axis_size("grid")
    members_k = lax.axis_size("kpt")
    planes = bands.shape[3]
    parts = jnp.asarray(np.stack(third_parts()))

    waves = bands[0].reshape(2, 2, planes, SIDE, SIDE).transpose(1, 2, 3, 0, 4)
    waves = waves.reshape(2, 2 * planes, HALF, USED)
    head, tail = waves[:, :9], waves[:, 9:]
    tail = tail.reshape(2, 3, HALF, 3, 32).transpose(0, 1, 3, 2, 4).reshape(2, 9, HALF, 32)
    packed = jnp.concatenate([head, tail], axis=-1)

    pairs = potential.reshape(planes // 2, 2, SIDE, SIDE).transpose(0, 2, 1, 3)
    pairs = pairs.reshape(planes // 2, SIDE, USED)
    pairs = jnp.pad(pairs, ((0, 0), (0, 0), (0, LANES - USED)))

    vmem = pl.BlockSpec(memory_space=pltpu.VMEM)
    total_planes = n * planes
    dma = pltpu.SemaphoreType.DMA
    out, energy, total = pl.pallas_call(
        functools.partial(kernel, n, members_k),
        name="cheb",
        out_shape=(
            jax.ShapeDtypeStruct((2, planes, SIDE, LANES), jnp.float32),
            jax.ShapeDtypeStruct((2, 8, LANES), jnp.float32),
            jax.ShapeDtypeStruct((8, LANES), jnp.float32),
        ),
        in_specs=[pl.BlockSpec(memory_space=pltpu.SMEM)] * 6 + [vmem] * 3,
        out_specs=(vmem, vmem, vmem),
        scratch_shapes=[
            pltpu.VMEM((total_planes + 2 * planes, ROWS, LANES), jnp.float32),
            pltpu.VMEM((total_planes + 2 * planes, ROWS, LANES), jnp.float32),
            pltpu.VMEM((total_planes + 2 * planes, ROWS, LANES), jnp.float32),
            pltpu.VMEM((2 * LANES, 2 * LANES), jnp.bfloat16),
            pltpu.VMEM((total_planes, SIDE, LANES), jnp.float32),
            pltpu.VMEM((n, 9, HALF, LANES), jnp.float32),
            pltpu.VMEM((n, planes // 2, SIDE, LANES), jnp.float32),
            pltpu.VMEM((n, 2, 8, LANES), jnp.float32),
            pltpu.VMEM((members_k, 8, LANES), jnp.float32),
            dma((5 + n,)),
            dma((n,)),
            dma((3 + 2 * n,)),
            dma((n,)),
            dma((n,)),
            dma((n,)),
            dma((members_k,)),
            dma((members_k,)),
            dma((2,)),
        ],
        compiler_params=pltpu.CompilerParams(
            collective_id=0, has_side_effects=True, vmem_limit_bytes=56 * 1024 * 1024
        ),
    )(table, kweight, lowest, cut, upper, fermi, packed, pairs, parts)
    filtered = out[..., :USED].reshape(2, planes, SIDE, 2, SIDE).transpose(3, 0, 1, 2, 4)
    filtered = filtered.reshape(1, 2, 2, planes, SIDE * SIDE)
    return filtered, energy[:, 0, 0][None], total[0, :1]


def solution(mesh):
    in_specs = (
        P("kpt", None, None, "grid", None),
        P("grid", None),
        P("kpt", None),
        P("kpt"),
        P("kpt"),
        P("kpt"),
        P("kpt"),
        P(),
    )
    out_specs = (P("kpt", None, None, "grid", None), P("kpt", None), P())
    return jax.shard_map(
        per_device, mesh=mesh, in_specs=in_specs, out_specs=out_specs, check_vma=False
    )
```
